32 devices in a mesh: patch: 16 (over z, x, core), lev: 2 (over y).
Axes of the slice: x: 2, y: 2, z: 4, core: 2. Of those that a mesh axis runs over, the one named last changes fastest.
Arguments:
- fields: bfloat16 [8, 32, 32768], P(None, 'lev', 'patch'), may hold values from -6 to 6
- interp: bfloat16 [128, 128, 256], P('patch'), may hold values from -0.375 to 0.375
- conv_weight: bfloat16 [128, 8, 128, 128], P('patch'), may hold values from -0.1875 to 0.1875
- vert_weight: float32 [32, 5], replicated, may hold values from 0.1 to 0.5
- send_tiles: int32 [16, 4, 2], P('patch'), may hold values from 0 to 8, as said below
- tile_pattern: int32 [128, 8], P('patch'), may hold values from 0 to 15, as said below
Outputs:
- localized: float32 [8, 32, 32768], P(None, 'lev', 'patch')
The draws below stay inside these ranges and needn't reach their ends.
Inputs may be any that keep to these rules, and one draw needn't show every extreme that they name: `send_tiles`: in every draw some link carries 2 tiles; every link carries at least one tile; the tiles of one link are distinct. `tile_pattern`: each row names distinct entries, each an own tile or a filled received slot.
All inputs are finite; a program needn't handle non-finite values.
Results may differ from the reference program's by a relative error of at most 0.0048.
Values may be sent and summed in bfloat16 or wider, within the bound.
A program may use at most 64 MiB of HBM per device.

```python
import math
import jax
import jax.numpy as jnp
from jax import lax

MEMBERS = 8
TILES_DEV = 8
TILE = 128
FINE_TILE = 256
K = 8
REACH = 2
MOST = 2
VHALF = 2
LEVELS = 32
BLOCKS = 128
COLUMNS = 32768
N_PATCH = 16


def link_table():
    return jnp.array([position - REACH if position < REACH else position - REACH + 1 for position in range(2 * REACH)], jnp.int32)


def link_counts(key):
    base = jax.random.fold_in(key, 11)
    counts = jax.random.randint(jax.random.fold_in(base, 1), (N_PATCH * 2 * REACH,), 1, MOST + 1)
    picked = jax.random.randint(jax.random.fold_in(base, 2), (), 0, N_PATCH * 2 * REACH)
    counts = jnp.where(jnp.arange(N_PATCH * 2 * REACH) == picked, MOST, counts)
    return counts.reshape(N_PATCH, 2 * REACH).astype(jnp.int32)


def draw_send_tiles(key, part):
    counts = link_counts(key)
    keys = jax.random.split(jax.random.fold_in(key, 12), N_PATCH * 2 * REACH)
    chosen = jax.vmap(lambda single: jax.random.permutation(single, TILES_DEV))(keys)[:, :MOST]
    chosen = chosen.reshape(N_PATCH, 2 * REACH, MOST)
    slot_ids = jnp.arange(MOST)[None, None, :]
    return jnp.where(slot_ids < counts[:, :, None], chosen, TILES_DEV).astype(jnp.int32)


def draw_tile_pattern(key, part):
    counts = link_counts(key)
    links = link_table()
    source = (jnp.arange(N_PATCH)[:, None] - links[None, :]) % N_PATCH
    arrived = counts[source, jnp.arange(2 * REACH)[None, :]]
    filled = jnp.arange(MOST)[None, None, :] < arrived[:, :, None]
    valid = jnp.concatenate([jnp.ones((N_PATCH, TILES_DEV), bool), filled.reshape(N_PATCH, 2 * REACH * MOST)], axis=1)
    width = TILES_DEV + 2 * REACH * MOST
    scores = jax.random.randint(jax.random.fold_in(key, 13), (N_PATCH, TILES_DEV, width), 0, 1 << 20) * width + jnp.arange(width)[None, None, :]
    scores = jnp.where(valid[:, None, :], scores, scores + (1 << 20) * width)
    order = jnp.argsort(scores, axis=-1)[..., :K]
    return order.reshape(N_PATCH * TILES_DEV, K).astype(jnp.int32)


def block_levels(stream_key, dims, shards, low, high):
    def one(dim, shards_of):
        heights = jax.random.uniform(jax.random.fold_in(jax.random.fold_in(stream_key, 6), dim), (shards_of,), jnp.float32, low / len(shards), high / len(shards))
        return jnp.repeat(jnp.exp(heights), dims[dim] // shards_of).reshape((-1,) + (1,) * (len(dims) - dim - 1))

    gain = one(*shards[0])
    for cut in shards[1:]:
        gain = gain * one(*cut)
    return gain


def noise(stream_key, extent, deviation, reach, cuts=(), kind=jnp.bfloat16):
    values = jax.random.normal(stream_key, extent, jnp.float32) * deviation
    if len(cuts) > 0:
        values = block_levels(stream_key, extent, cuts, -0.22, 0.18) * values
    return jnp.clip(values, min=-reach, max=reach).astype(kind)


def setup_inputs(seed: int = 0) -> dict:
    key_list = jax.random.split(jax.random.key(seed), 7)
    return {
        "fields": noise(key_list[0], (MEMBERS, LEVELS, COLUMNS), 1.0, 6.0, ((1, 2), (2, 16))),
        "interp": noise(key_list[1], (BLOCKS, TILE, FINE_TILE), FINE_TILE ** -0.5, 0.375, ((0, 16),)),
        "conv_weight": noise(key_list[2], (BLOCKS, K, TILE, TILE), (K * TILE) ** -0.5, 0.1875, ((0, 16),)),
        "vert_weight": jnp.clip(jnp.exp(jax.random.uniform(key_list[3], (LEVELS, 2 * VHALF + 1), jnp.float32, math.log(0.1), math.log(0.5))), 0.1, 0.5),
        "send_tiles": draw_send_tiles(jax.random.fold_in(key_list[6], 71), 0),
        "tile_pattern": draw_tile_pattern(jax.random.fold_in(key_list[6], 71), 0),
    }


HIGHEST = lax.Precision.HIGHEST


def link_offsets(reach_len):
    return [position - reach_len if position < reach_len else position - reach_len + 1 for position in range(2 * reach_len)]


def vertical_adjoint(values, weights, length, half_width):
    summed = jnp.zeros(values.shape[:-2] + (length, values.shape[-1]), jnp.float32)
    for offset in range(-half_width, half_width + 1):
        factor = weights[half_width + offset: half_width + offset + length, half_width - offset]
        summed = summed + factor[:, None] * values[..., half_width + offset: half_width + offset + length, :].astype(jnp.float32)
    return summed


def vertical_forward(values, weights, length, half_width):
    summed = jnp.zeros(values.shape[:-2] + (length, values.shape[-1]), jnp.float32)
    for offset in range(2 * half_width + 1):
        factor = weights[half_width: half_width + length, offset]
        summed = summed + factor[:, None] * values[..., offset: offset + length, :].astype(jnp.float32)
    return summed


def reference(fields, interp, conv_weight, vert_weight, send_tiles, tile_pattern):
    members, level_total, column_total = fields.shape
    block_total, tile_len, fine_len = interp.shape
    patch_count = N_PATCH
    tile_count = block_total // patch_count
    reach_len = send_tiles.shape[1] // 2
    slot_most = send_tiles.shape[2]
    half_width = (vert_weight.shape[1] - 1) // 2
    row_count = members * level_total
    extended_len = tile_count + 2 * reach_len * slot_most
    offsets = link_offsets(reach_len)
    flat = fields.reshape(row_count, patch_count, tile_count, fine_len)
    interp_patch = interp.reshape(patch_count, tile_count, tile_len, fine_len)
    conv_patch = conv_weight.reshape(patch_count, tile_count, -1, tile_len, tile_len)
    pattern_patch = tile_pattern.reshape(patch_count, tile_count, -1)
    positions = jnp.arange(patch_count).astype(jnp.int32)

    def restrict(position):
        block = lax.dynamic_index_in_dim(flat, position, 1, keepdims=False)
        return jnp.einsum("rtf,tcf->trc", block.astype(jnp.float32), interp_patch[position].astype(jnp.float32), precision=HIGHEST).astype(jnp.bfloat16)

    coarse = lax.map(restrict, positions)

    def adjoint_patch(position):
        products = jnp.einsum("tro,tkio->tkri", coarse[position].astype(jnp.float32), conv_patch[position].astype(jnp.float32), precision=HIGHEST)
        chosen = (pattern_patch[position][:, :, None] == jnp.arange(extended_len).astype(jnp.int32)[None, None, :]).astype(jnp.float32)
        summed = jnp.einsum("tke,tkri->eri", chosen, products, precision=HIGHEST)
        returning = summed[tile_count:].reshape(2 * reach_len, slot_most, row_count, tile_len).astype(jnp.bfloat16)
        return summed[:tile_count], returning

    own_part, returning = lax.map(adjoint_patch, positions)
    arrived_back = jnp.stack([jnp.roll(returning[:, position], -offsets[position], axis=0) for position in range(2 * reach_len)], axis=1)

    def combine(position):
        sending = (send_tiles[position][:, :, None] == jnp.arange(tile_count).astype(jnp.int32)[None, None, :]).astype(jnp.float32)
        added = jnp.einsum("ost,osri->tri", sending, arrived_back[position].astype(jnp.float32), precision=HIGHEST)
        return (own_part[position] + added).astype(jnp.bfloat16)

    adjoint = lax.map(combine, positions).reshape(patch_count, tile_count, members, level_total, tile_len)
    level_pad = ((0, 0), (0, 0), (0, 0), (half_width, half_width), (0, 0))
    weight_pad = jnp.pad(vert_weight, ((half_width, half_width), (0, 0)))
    middle = vertical_adjoint(jnp.pad(adjoint, level_pad), weight_pad, level_total, half_width).astype(jnp.bfloat16)
    smooth = vertical_forward(jnp.pad(middle, level_pad), weight_pad, level_total, half_width).astype(jnp.bfloat16)
    smooth = smooth.reshape(patch_count, tile_count, row_count, tile_len)

    def pack(position):
        sending = (send_tiles[position][:, :, None] == jnp.arange(tile_count).astype(jnp.int32)[None, None, :]).astype(jnp.float32)
        return jnp.einsum("ost,tri->osri", sending, smooth[position].astype(jnp.float32), precision=HIGHEST).astype(jnp.bfloat16)

    slots = lax.map(pack, positions)
    arrived = jnp.stack([jnp.roll(slots[:, position], offsets[position], axis=0) for position in range(2 * reach_len)], axis=1)

    def forward_patch(position):
        extended = jnp.concatenate([smooth[position], arrived[position].reshape(-1, row_count, tile_len)], axis=0)
        chosen = (pattern_patch[position][:, :, None] == jnp.arange(extended_len).astype(jnp.int32)[None, None, :]).astype(jnp.float32)
        picked = jnp.einsum("tke,eri->tkri", chosen, extended.astype(jnp.float32), precision=HIGHEST)
        mixed = jnp.einsum("tkri,tkio->tro", picked, conv_patch[position].astype(jnp.float32), precision=HIGHEST).astype(jnp.bfloat16)
        return jnp.einsum("tro,tof->rtf", mixed.astype(jnp.float32), interp_patch[position].astype(jnp.float32), precision=HIGHEST)

    result = lax.map(forward_patch, positions)
    return jnp.transpose(result, (1, 0, 2, 3)).reshape(members, level_total, column_total)
```

```python
import functools

import jax
import jax.numpy as jnp
from jax import lax
from jax.experimental import pallas as pl
from jax.experimental.pallas import tpu as pltpu
from jax.sharding import PartitionSpec as P

MESH = pl.DeviceIdType.MESH
F32 = jnp.float32
BF16 = jnp.bfloat16


def link_offsets(reach_len):
    return [
        position - reach_len if position < reach_len else position - reach_len + 1
        for position in range(2 * reach_len)
    ]


def dot_t(left, right):
    return lax.dot_general(left, right, (((1,), (1,)), ((), ())), preferred_element_type=F32)


def kernel(
    n_patch,
    n_lev,
    fields_hbm,
    interp_hbm,
    conv_hbm,
    weight,
    send,
    pattern,
    out_hbm,
    fields,
    interp,
    conv,
    coarse,
    levels,
    middle,
    halo_out,
    halo_in,
    smooth,
    own,
    ext,
    mixed,
    out,
    which,
    slot_of,
    load_sem,
    out_sem,
    halo_sem,
    back_sem,
    forth_sem,
    *links,
):
    members, level_len, _ = fields.shape
    tiles, tile_len, fine = interp.shape
    k_len = conv_hbm.shape[1]
    link_len, most = send.shape[1], send.shape[2]
    half = (weight.shape[1] - 1) // 2
    wide = 2 * half
    rows = members * level_len
    total_levels = weight.shape[0]
    offsets = link_offsets(link_len // 2)
    returning, arrived_back, sending, arrived = (
        links[i * link_len : (i + 1) * link_len] for i in range(4)
    )
    me_p, me_l = lax.axis_index("patch"), lax.axis_index("lev")
    partner = [lax.rem(me_p + d + n_patch, n_patch) for d in offsets]
    source = [lax.rem(me_p - d + n_patch, n_patch) for d in offsets]
    order = sorted(range(link_len), key=lambda o: -abs(offsets[o]))

    load_f = pltpu.make_async_copy(fields_hbm, fields, load_sem.at[0])
    load_i = pltpu.make_async_copy(interp_hbm, interp, load_sem.at[1])
    load_c = pltpu.make_async_copy(conv_hbm, conv.at[:, pl.ds(0, k_len)], load_sem.at[2])
    load_f.start()
    load_i.start()
    load_c.start()

    barrier = pltpu.get_barrier_semaphore()
    for other in partner:
        pl.semaphore_signal(barrier, inc=1, device_id={"patch": other}, device_id_type=MESH)

    @pl.when(me_l > 0)
    def _():
        pl.semaphore_signal(barrier, inc=1, device_id={"lev": me_l - 1}, device_id_type=MESH)

    @pl.when(me_l < n_lev - 1)
    def _():
        pl.semaphore_signal(barrier, inc=1, device_id={"lev": me_l + 1}, device_id_type=MESH)

    @pl.loop(0, tiles)
    def _(t):
        named = [pattern[t, k] for k in range(k_len)]
        for e in range(tiles + link_len * most):
            index = jnp.int32(k_len)
            for k in range(k_len):
                index = jnp.where(named[k] == e, k, index)
            which[t, e] = index
        for o in range(link_len):
            index = jnp.int32(most)
            for s in range(most):
                index = jnp.where(send[0, o, s] == t, s, index)
            slot_of[t, o] = index
        conv[t, k_len] = jnp.zeros((tile_len, tile_len), BF16)

    for o in range(link_len):
        arrived_back[o][most] = jnp.zeros((rows, tile_len), BF16)
    ext[tiles] = jnp.zeros((rows, tile_len), BF16)

    load_f.wait()
    load_i.wait()
    for t in range(tiles):
        block = fields[:, :, t * fine : (t + 1) * fine].reshape(rows, fine)
        coarse[t] = dot_t(block, interp[t])
        for l in range(level_len):
            levels[wide + l, t] = coarse[t, pl.ds(l, members, stride=level_len), :]
    for i in range(wide // 2):
        low = jnp.concatenate([levels[wide + 2 * i], levels[wide + 2 * i + 1]], axis=1)
        top = level_len + 2 * i
        high = jnp.concatenate([levels[top], levels[top + 1]], axis=1)
        halo_out[0, i] = low.astype(BF16)
        halo_out[1, i] = high.astype(BF16)

    down = pltpu.make_async_remote_copy(
        halo_out.at[0],
        halo_in.at[1],
        halo_sem.at[0],
        halo_sem.at[1],
        device_id={"lev": lax.rem(me_l + n_lev - 1, n_lev)},
        device_id_type=MESH,
    )
    up = pltpu.make_async_remote_copy(
        halo_out.at[1],
        halo_in.at[0],
        halo_sem.at[2],
        halo_sem.at[3],
        device_id={"lev": lax.rem(me_l + 1, n_lev)},
        device_id_type=MESH,
    )
    beside = jnp.where(me_l > 0, 1, 0) + jnp.where(me_l < n_lev - 1, 1, 0)
    pl.semaphore_wait(barrier, link_len + beside)

    @pl.when(me_l > 0)
    def _():
        down.start()

    @pl.when(me_l < n_lev - 1)
    def _():
        up.start()

    start = me_l * level_len

    def coefficient(level, column):
        return weight[jnp.clip(start + level, 0, total_levels - 1), column]

    def adjoint_level(level):
        value = coefficient(level - half, wide) * levels[wide + level - half]
        for e in range(1 - half, half + 1):
            value = value + coefficient(level + e, half - e) * levels[wide + level + e]
        if level < 0:
            value = jnp.where(start + level >= 0, value, 0.0)
        if level >= level_len:
            value = jnp.where(start + level < total_levels, value, 0.0)
        middle[half + level] = value

    def forward_pair(level):
        both = []
        for l in (level, level + 1):
            value = coefficient(l, 0) * middle[l]
            for j in range(1, wide + 1):
                value = value + coefficient(l, j) * middle[l + j]
            both.append(value)
        smooth[:, level * members : (level + 2) * members, :] = jnp.concatenate(
            both, axis=1
        ).astype(BF16)

    for level in range(half, level_len - half):
        adjoint_level(level)
    for level in range(wide, level_len - wide, 2):
        forward_pair(level)

    def unpack(side, base):
        for i in range(wide // 2):
            pair = halo_in[side, i].astype(F32)
            levels[base + 2 * i] = pair[:, :members]
            levels[base + 2 * i + 1] = pair[:, members:]

    def clear(base):
        for i in range(wide):
            levels[base + i] = jnp.zeros(levels.shape[1:], F32)

    @pl.when(me_l > 0)
    def _():
        up.wait_recv()
        unpack(0, 0)

    @pl.when(me_l == 0)
    def _():
        clear(0)

    @pl.when(me_l < n_lev - 1)
    def _():
        down.wait_recv()
        unpack(1, wide + level_len)

    @pl.when(me_l == n_lev - 1)
    def _():
        clear(wide + level_len)

    for level in list(range(-half, half)) + list(range(level_len - half, level_len + half)):
        adjoint_level(level)
    for level in list(range(0, wide, 2)) + list(range(level_len - wide, level_len, 2)):
        forward_pair(level)

    load_c.wait()

    def gathered(first):
        left = jnp.concatenate([smooth[t] for t in range(tiles)], axis=1)
        right = jnp.concatenate(
            [
                jnp.concatenate([conv[t, which[t, first + s]] for t in range(tiles)], axis=1)
                for s in range(most)
            ],
            axis=0,
        )
        return dot_t(left, right)

    back = []
    for o in order:
        sums = gathered(tiles + o * most).astype(BF16)
        for s in range(most):
            returning[o][s] = sums[:, s * tile_len : (s + 1) * tile_len]
        copy = pltpu.make_async_remote_copy(
            returning[o],
            arrived_back[o].at[pl.ds(0, most)],
            back_sem.at[0, o],
            back_sem.at[1, o],
            device_id={"patch": source[o]},
            device_id_type=MESH,
        )
        copy.start()
        back.append(copy)
    for first in range(0, tiles, most):
        sums = gathered(first)
        for s in range(most):
            own[first + s] = sums[:, s * tile_len : (s + 1) * tile_len]
    for copy in back:
        copy.wait_recv()
    for t in range(tiles):
        value = own[t]
        for o in range(link_len):
            value = value + arrived_back[o][slot_of[t, o]].astype(F32)
        ext[t] = value.astype(BF16)
    forth = []
    for o in order:
        for s in range(most):
            sending[o][s] = ext[send[0, o, s]]
        copy = pltpu.make_async_remote_copy(
            sending[o],
            arrived[o],
            forth_sem.at[0, o],
            forth_sem.at[1, o],
            device_id={"patch": partner[o]},
            device_id_type=MESH,
        )
        copy.start()
        forth.append(copy)

    def spread(left, first, count, t):
        right = jnp.concatenate(
            [
                jnp.concatenate([conv[u, which[u, first + e]] for e in range(count)], axis=0)
                for u in (t, t + 1)
            ],
            axis=1,
        )
        return jnp.dot(left, right, preferred_element_type=F32)

    left = jnp.concatenate([ext[e] for e in range(tiles)], axis=1)
    for t in range(0, tiles, 2):
        sums = spread(left, 0, tiles, t)
        mixed[t] = sums[:, :tile_len]
        mixed[t + 1] = sums[:, tile_len:]
    near = order[::-1]
    for o in near:
        forth[order.index(o)].wait_recv()
        left = jnp.concatenate([arrived[o][s] for s in range(most)], axis=1)
        for t in range(0, tiles, 2):
            sums = spread(left, tiles + o * most, most, t)
            mixed[t] = mixed[t] + sums[:, :tile_len]
            mixed[t + 1] = mixed[t + 1] + sums[:, tile_len:]
    stores = []
    for t in range(tiles):
        part = jnp.concatenate(
            [mixed[t, pl.ds(m, level_len, stride=members), :] for m in range(members)], axis=0
        ).astype(BF16)
        result = jnp.dot(part, interp[t], preferred_element_type=F32)
        columns = pl.ds(t * fine, fine)
        out[:, :, columns] = result.reshape(members, level_len, fine)
        store = pltpu.make_async_copy(
            out.at[:, :, columns], out_hbm.at[:, :, columns], out_sem.at[t]
        )
        store.start()
        stores.append(store)
    for copy in back + forth:
        copy.wait_send()

    @pl.when(me_l > 0)
    def _():
        down.wait_send()

    @pl.when(me_l < n_lev - 1)
    def _():
        up.wait_send()

    for store in stores:
        store.wait()


def solution(mesh):
    n_patch, n_lev = mesh.shape["patch"], mesh.shape["lev"]

    def shards(fields, interp, conv_weight, vert_weight, send_tiles, tile_pattern):
        members, level_len, column_len = fields.shape
        tiles, tile_len, fine = interp.shape
        k_len = conv_weight.shape[1]
        link_len, most = send_tiles.shape[1:]
        wide = vert_weight.shape[1] - 1
        rows = members * level_len
        any_spec = pl.BlockSpec(memory_space=pl.ANY)
        smem_spec = pl.BlockSpec(memory_space=pltpu.SMEM)

        def per_link(count):
            return [pltpu.VMEM((count, rows, tile_len), BF16) for _ in range(link_len)]

        return pl.pallas_call(
            functools.partial(kernel, n_patch, n_lev),
            name="localize",
            out_shape=jax.ShapeDtypeStruct(fields.shape, F32),
            in_specs=[any_spec] * 3 + [smem_spec] * 3,
            out_specs=any_spec,
            scratch_shapes=[
                pltpu.VMEM(fields.shape, BF16),
                pltpu.VMEM(interp.shape, BF16),
                pltpu.VMEM((tiles, k_len + 1, tile_len, tile_len), BF16),
                pltpu.VMEM((tiles, rows, tile_len), F32),
                pltpu.VMEM((level_len + 2 * wide, tiles, members, tile_len), F32),
                pltpu.VMEM((level_len + wide, tiles, members, tile_len), F32),
                pltpu.VMEM((2, wide // 2, tiles, 2 * members, tile_len), BF16),
                pltpu.VMEM((2, wide // 2, tiles, 2 * members, tile_len), BF16),
                pltpu.VMEM((tiles, rows, tile_len), BF16),
                pltpu.VMEM((tiles, rows, tile_len), F32),
                pltpu.VMEM((tiles + 1, rows, tile_len), BF16),
                pltpu.VMEM((tiles, rows, tile_len), F32),
                pltpu.VMEM(fields.shape, F32),
                pltpu.SMEM((tiles, tiles + link_len * most), jnp.int32),
                pltpu.SMEM((tiles, link_len), jnp.int32),
                pltpu.SemaphoreType.DMA((3,)),
                pltpu.SemaphoreType.DMA((tiles,)),
                pltpu.SemaphoreType.DMA((4,)),
                pltpu.SemaphoreType.DMA((2, link_len)),
                pltpu.SemaphoreType.DMA((2, link_len)),
            ]
            + per_link(most)
            + per_link(most + 1)
            + per_link(most)
            + per_link(most),
            compiler_params=pltpu.CompilerParams(collective_id=0, has_side_effects=True),
        )(fields, interp, conv_weight, vert_weight, send_tiles, tile_pattern)

    in_specs = (
        P(None, "lev", "patch"),
        P("patch", None, None),
        P("patch", None, None, None),
        P(),
        P("patch", None, None),
        P("patch", None),
    )
    out_specs = P(None, "lev", "patch")
    return jax.shard_map(shards, mesh=mesh, in_specs=in_specs, out_specs=out_specs, check_vma=False)
```

```python
import functools

import jax
import jax.numpy as jnp
from jax import lax
from jax.experimental import pallas as pl
from jax.experimental.pallas import tpu as pltpu
from jax.sharding import PartitionSpec as P

MESH = pl.DeviceIdType.MESH
F32 = jnp.float32
BF16 = jnp.bfloat16


def link_offsets(reach_len):
    return [
        position - reach_len if position < reach_len else position - reach_len + 1
        for position in range(2 * reach_len)
    ]


def dot_t(left, right):
    return lax.dot_general(left, right, (((1,), (1,)), ((), ())), preferred_element_type=F32)


def kernel(
    n_patch,
    n_lev,
    fields_hbm,
    interp_hbm,
    conv_hbm,
    weight,
    send,
    pattern,
    out,
    fields,
    interp,
    conv,
    coarse,
    levels,
    middle,
    halo_out,
    halo_in,
    own,
    mixed,
    which,
    slot_of,
    load_sem,
    halo_sem,
    back_sem,
    forth_sem,
    *parts,
):
    members, level_len, _ = fields.shape
    tiles, tile_len, fine = interp.shape
    k_len = conv_hbm.shape[1]
    most, link_len = send.shape[1], send.shape[2]
    half = (weight.shape[0] - 1) // 2
    wide = 2 * half
    rows = members * level_len
    total_levels = weight.shape[1]
    offsets = link_offsets(link_len // 2)
    smooth, ext, links = parts[:2], parts[2:4], parts[4:]
    returning, arrived_back, sending, arrived = (
        [links[(2 * i + c) * link_len : (2 * i + c + 1) * link_len] for c in range(2)]
        for i in range(4)
    )
    edge = wide * members
    part_rows = (rows - 2 * edge, 2 * edge)
    me_p, me_l = lax.axis_index("patch"), lax.axis_index("lev")
    partner = [lax.rem(me_p + d + n_patch, n_patch) for d in offsets]
    source = [lax.rem(me_p - d + n_patch, n_patch) for d in offsets]
    order = sorted(range(link_len), key=lambda o: -abs(offsets[o]))

    load_f = pltpu.make_async_copy(fields_hbm, fields, load_sem.at[0])
    load_i = pltpu.make_async_copy(interp_hbm, interp, load_sem.at[1])
    load_c = pltpu.make_async_copy(conv_hbm, conv.at[:, pl.ds(0, k_len)], load_sem.at[2])
    load_f.start()
    load_i.start()

    barrier = pltpu.get_barrier_semaphore()
    for other in partner:
        pl.semaphore_signal(barrier, inc=1, device_id={"patch": other}, device_id_type=MESH)

    @pl.when(me_l > 0)
    def _():
        pl.semaphore_signal(barrier, inc=1, device_id={"lev": me_l - 1}, device_id_type=MESH)

    @pl.when(me_l < n_lev - 1)
    def _():
        pl.semaphore_signal(barrier, inc=1, device_id={"lev": me_l + 1}, device_id_type=MESH)

    @pl.loop(0, tiles)
    def _(t):
        named = [pattern[t, k] for k in range(k_len)]
        for e in range(tiles + link_len * most):
            index = jnp.int32(k_len)
            for k in range(k_len):
                index = jnp.where(named[k] == e, k, index)
            which[t, e] = index
        for o in range(link_len):
            index = jnp.int32(most)
            for s in range(most):
                index = jnp.where(send[0, s, o] == t, s, index)
            slot_of[t, o] = index
        conv[t, k_len] = jnp.zeros((tile_len, tile_len), BF16)

    load_c.start()
    for c in range(2):
        for o in range(link_len):
            arrived_back[c][o][most] = jnp.zeros((part_rows[c], tile_len), BF16)
        ext[c][tiles] = jnp.zeros((part_rows[c], tile_len), BF16)

    load_f.wait()
    load_i.wait()
    for t in range(tiles):
        block = fields[:, :, t * fine : (t + 1) * fine].reshape(rows, fine)
        coarse[t] = dot_t(block, interp[t])
        for l in range(level_len):
            levels[wide + l, t] = coarse[t, pl.ds(l, members, stride=level_len), :]
    for i in range(wide // 2):
        low = jnp.concatenate([levels[wide + 2 * i], levels[wide + 2 * i + 1]], axis=1)
        top = level_len + 2 * i
        high = jnp.concatenate([levels[top], levels[top + 1]], axis=1)
        halo_out[0, i] = low.astype(BF16)
        halo_out[1, i] = high.astype(BF16)

    down = pltpu.make_async_remote_copy(
        halo_out.at[0],
        halo_in.at[1],
        halo_sem.at[0],
        halo_sem.at[1],
        device_id={"lev": lax.rem(me_l + n_lev - 1, n_lev)},
        device_id_type=MESH,
    )
    up = pltpu.make_async_remote_copy(
        halo_out.at[1],
        halo_in.at[0],
        halo_sem.at[2],
        halo_sem.at[3],
        device_id={"lev": lax.rem(me_l + 1, n_lev)},
        device_id_type=MESH,
    )
    beside = jnp.where(me_l > 0, 1, 0) + jnp.where(me_l < n_lev - 1, 1, 0)
    pl.semaphore_wait(barrier, link_len + beside)

    @pl.when(me_l > 0)
    def _():
        down.start()

    @pl.when(me_l < n_lev - 1)
    def _():
        up.start()

    start = me_l * level_len

    def coefficient(level, column):
        return weight[column, jnp.clip(start + level, 0, total_levels - 1)]

    def adjoint_level(level):
        value = coefficient(level - half, wide) * levels[wide + level - half]
        for e in range(1 - half, half + 1):
            value = value + coefficient(level + e, half - e) * levels[wide + level + e]
        if level < 0:
            value = jnp.where(start + level >= 0, value, 0.0)
        if level >= level_len:
            value = jnp.where(start + level < total_levels, value, 0.0)
        middle[half + level] = value

    def forward_pair(level):
        both = []
        for l in (level, level + 1):
            value = coefficient(l, 0) * middle[l]
            for j in range(1, wide + 1):
                value = value + coefficient(l, j) * middle[l + j]
            both.append(value)
        pair = jnp.concatenate(both, axis=1).astype(BF16)
        if wide <= level < level_len - wide:
            smooth[0][:, pl.ds((level - wide) * members, 2 * members), :] = pair
        else:
            place = level if level < wide else level - level_len + 2 * wide
            smooth[1][:, pl.ds(place * members, 2 * members), :] = pair

    for level in range(half, level_len - half):
        adjoint_level(level)
    for level in range(wide, level_len - wide, 2):
        forward_pair(level)

    load_c.wait()

    def gathered(left, first):
        right = jnp.concatenate(
            [
                jnp.concatenate([conv[t, which[t, first + s]] for t in range(tiles)], axis=1)
                for s in range(most)
            ],
            axis=0,
        )
        return dot_t(left, right)

    def side_by_side(ref, count):
        return jnp.concatenate([ref[i] for i in range(count)], axis=1)

    def send_back(c):
        left = side_by_side(smooth[c], tiles)
        copies = {}
        for o in order:
            sums = gathered(left, tiles + o * most).astype(BF16)
            for s in range(most):
                returning[c][o][s] = sums[:, s * tile_len : (s + 1) * tile_len]
            copies[o] = pltpu.make_async_remote_copy(
                returning[c][o],
                arrived_back[c][o].at[pl.ds(0, most)],
                back_sem.at[0, c, o],
                back_sem.at[1, c, o],
                device_id={"patch": source[o]},
                device_id_type=MESH,
            )
            copies[o].start()
        return copies

    def send_forth(c):
        low = 0 if c == 0 else part_rows[0]
        for t in range(tiles):
            value = own[t, low : low + part_rows[c]]
            for o in range(link_len):
                value = value + arrived_back[c][o][slot_of[t, o]].astype(F32)
            ext[c][t] = value.astype(BF16)
        copies = {}
        for o in order:
            for s in range(most):
                sending[c][o][s] = ext[c][send[0, s, o]]
            copies[o] = pltpu.make_async_remote_copy(
                sending[c][o],
                arrived[c][o],
                forth_sem.at[0, c, o],
                forth_sem.at[1, c, o],
                device_id={"patch": partner[o]},
                device_id_type=MESH,
            )
            copies[o].start()
        return copies

    def spread(left, first, count, t):
        right = jnp.concatenate(
            [
                jnp.concatenate([conv[u, which[u, first + e]] for e in range(count)], axis=0)
                for u in (t, t + 1)
            ],
            axis=1,
        )
        return jnp.dot(left, right, preferred_element_type=F32)

    def places(c):
        if c == 0:
            return [(0, part_rows[0], edge)]
        return [(0, edge, 0), (edge, edge, rows - edge)]

    def put(c, t, sums, fresh):
        for begin, count, place in places(c):
            for i in range(2):
                value = sums[begin : begin + count, i * tile_len : (i + 1) * tile_len]
                if not fresh:
                    value = value + mixed[t + i, pl.ds(place, count)]
                mixed[t + i, pl.ds(place, count)] = value

    def mix_own(c):
        left = side_by_side(ext[c], tiles)
        for t in range(0, tiles, 2):
            put(c, t, spread(left, 0, tiles, t), True)

    def mix_link(c, o):
        left = side_by_side(arrived[c][o], most)
        for t in range(0, tiles, 2):
            put(c, t, spread(left, tiles + o * most, most, t), False)

    back = [send_back(0)]

    def unpack(side, base):
        for i in range(wide // 2):
            pair = halo_in[side, i].astype(F32)
            levels[base + 2 * i] = pair[:, :members]
            levels[base + 2 * i + 1] = pair[:, members:]

    def clear(base):
        for i in range(wide):
            levels[base + i] = jnp.zeros(levels.shape[1:], F32)

    @pl.when(me_l > 0)
    def _():
        up.wait_recv()
        unpack(0, 0)

    @pl.when(me_l == 0)
    def _():
        clear(0)

    @pl.when(me_l < n_lev - 1)
    def _():
        down.wait_recv()
        unpack(1, wide + level_len)

    @pl.when(me_l == n_lev - 1)
    def _():
        clear(wide + level_len)

    for level in list(range(-half, half)) + list(range(level_len - half, level_len + half)):
        adjoint_level(level)
    for level in list(range(0, wide, 2)) + list(range(level_len - wide, level_len, 2)):
        forward_pair(level)

    back.append(send_back(1))
    left = jnp.concatenate([side_by_side(smooth[c], tiles) for c in range(2)], axis=0)
    for first in range(0, tiles, most):
        sums = gathered(left, first)
        for s in range(most):
            own[first + s] = sums[:, s * tile_len : (s + 1) * tile_len]
    forth = []
    for c in range(2):
        for o in order:
            back[c][o].wait_recv()
        forth.append(send_forth(c))
        mix_own(c)
    for c in range(2):
        for o in order[::-1]:
            forth[c][o].wait_recv()
            mix_link(c, o)
    for t in range(tiles):
        part = jnp.concatenate(
            [mixed[t, pl.ds(m, level_len, stride=members), :] for m in range(members)], axis=0
        ).astype(BF16)
        result = jnp.dot(part, interp[t], preferred_element_type=F32)
        out[:, :, t * fine : (t + 1) * fine] = result.reshape(members, level_len, fine)
    for copies in back + forth:
        for o in order:
            copies[o].wait_send()

    @pl.when(me_l > 0)
    def _():
        down.wait_send()

    @pl.when(me_l < n_lev - 1)
    def _():
        up.wait_send()


def solution(mesh):
    n_patch, n_lev = mesh.shape["patch"], mesh.shape["lev"]

    def shards(fields, interp, conv_weight, vert_weight, send_tiles, tile_pattern):
        members, level_len, column_len = fields.shape
        tiles, tile_len, fine = interp.shape
        k_len = conv_weight.shape[1]
        link_len, most = send_tiles.shape[1:]
        wide = vert_weight.shape[1] - 1
        rows = members * level_len
        any_spec = pl.BlockSpec(memory_space=pl.ANY)
        smem_spec = pl.BlockSpec(memory_space=pltpu.SMEM)

        edge = 2 * wide * members

        def per_part(count, copies):
            return [
                pltpu.VMEM((count, part_rows, tile_len), BF16)
                for part_rows in (rows - edge, edge)
                for _ in range(copies)
            ]

        return pl.pallas_call(
            functools.partial(kernel, n_patch, n_lev),
            name="localize",
            out_shape=pltpu.VMEM(fields.shape, F32),
            in_specs=[any_spec] * 3 + [smem_spec] * 3,
            out_specs=pl.BlockSpec(memory_space=pltpu.VMEM),
            scratch_shapes=[
                pltpu.VMEM(fields.shape, BF16),
                pltpu.VMEM(interp.shape, BF16),
                pltpu.VMEM((tiles, k_len + 1, tile_len, tile_len), BF16),
                pltpu.VMEM((tiles, rows, tile_len), F32),
                pltpu.VMEM((level_len + 2 * wide, tiles, members, tile_len), F32),
                pltpu.VMEM((level_len + wide, tiles, members, tile_len), F32),
                pltpu.VMEM((2, wide // 2, tiles, 2 * members, tile_len), BF16),
                pltpu.VMEM((2, wide // 2, tiles, 2 * members, tile_len), BF16),
                pltpu.VMEM((tiles, rows, tile_len), F32),
                pltpu.VMEM((tiles, rows, tile_len), F32),
                pltpu.SMEM((tiles, tiles + link_len * most), jnp.int32),
                pltpu.SMEM((tiles, link_len), jnp.int32),
                pltpu.SemaphoreType.DMA((3,)),
                pltpu.SemaphoreType.DMA((4,)),
                pltpu.SemaphoreType.DMA((2, 2, link_len)),
                pltpu.SemaphoreType.DMA((2, 2, link_len)),
            ]
            + per_part(tiles, 1)
            + per_part(tiles + 1, 1)
            + per_part(most, link_len)
            + per_part(most + 1, link_len)
            + per_part(most, link_len)
            + per_part(most, link_len),
            compiler_params=pltpu.CompilerParams(collective_id=0, has_side_effects=True),
        )(fields, interp, conv_weight, vert_weight.T, send_tiles.transpose(0, 2, 1), tile_pattern)

    in_specs = (
        P(None, "lev", "patch"),
        P("patch", None, None),
        P("patch", None, None, None),
        P(),
        P("patch", None, None),
        P("patch", None),
    )
    out_specs = P(None, "lev", "patch")
    return jax.shard_map(shards, mesh=mesh, in_specs=in_specs, out_specs=out_specs, check_vma=False)
```

```python
import functools

import jax
import jax.numpy as jnp
from jax import lax
from jax.experimental import pallas as pl
from jax.experimental.pallas import tpu as pltpu
from jax.sharding import PartitionSpec as P

MESH = pl.DeviceIdType.MESH
F32 = jnp.float32
BF16 = jnp.bfloat16


def link_offsets(reach_len):
    return [
        position - reach_len if position < reach_len else position - reach_len + 1
        for position in range(2 * reach_len)
    ]


def dot_t(left, right):
    return lax.dot_general(left, right, (((1,), (1,)), ((), ())), preferred_element_type=F32)


def kernel(
    n_patch,
    n_lev,
    fields_hbm,
    interp_hbm,
    conv_hbm,
    weight,
    send,
    pattern,
    out,
    fields,
    interp,
    conv,
    coarse,
    levels,
    middle,
    halo_out,
    halo_in,
    own,
    mixed,
    which,
    slot_of,
    load_sem,
    halo_sem,
    back_sem,
    forth_sem,
    *parts,
):
    members, level_len, _ = fields.shape
    tiles, tile_len, fine = interp.shape
    k_len = conv_hbm.shape[1]
    most, link_len = send.shape[1], send.shape[2]
    half = (weight.shape[0] - 1) // 2
    wide = 2 * half
    rows = members * level_len
    total_levels = weight.shape[1]
    offsets = link_offsets(link_len // 2)
    smooth, ext, links = parts[:2], parts[2:4], parts[4:]
    returning, arrived_back, sending, arrived = (
        [links[(2 * i + c) * link_len : (2 * i + c + 1) * link_len] for c in range(2)]
        for i in range(4)
    )
    edge = wide * members
    part_rows = (rows - 2 * edge, 2 * edge)
    me_p, me_l = lax.axis_index("patch"), lax.axis_index("lev")
    partner = [lax.rem(me_p + d + n_patch, n_patch) for d in offsets]
    source = [lax.rem(me_p - d + n_patch, n_patch) for d in offsets]
    order = sorted(range(link_len), key=lambda o: -abs(offsets[o]))

    load_f = pltpu.make_async_copy(fields_hbm, fields, load_sem.at[0])
    load_i = pltpu.make_async_copy(interp_hbm, interp, load_sem.at[1])
    load_c = pltpu.make_async_copy(conv_hbm, conv.at[:, pl.ds(0, k_len)], load_sem.at[2])
    load_f.start()
    load_i.start()

    barrier = pltpu.get_barrier_semaphore()
    for other in partner:
        pl.semaphore_signal(barrier, inc=1, device_id={"patch": other}, device_id_type=MESH)

    @pl.when(me_l > 0)
    def _():
        pl.semaphore_signal(barrier, inc=1, device_id={"lev": me_l - 1}, device_id_type=MESH)

    @pl.when(me_l < n_lev - 1)
    def _():
        pl.semaphore_signal(barrier, inc=1, device_id={"lev": me_l + 1}, device_id_type=MESH)

    @pl.loop(0, tiles)
    def _(t):
        named = [pattern[t, k] for k in range(k_len)]
        for e in range(tiles + link_len * most):
            index = jnp.int32(k_len)
            for k in range(k_len):
                index = jnp.where(named[k] == e, k, index)
            which[t, e] = index
        for o in range(link_len):
            index = jnp.int32(most)
            for s in range(most):
                index = jnp.where(send[0, s, o] == t, s, index)
            slot_of[t, o] = index
        conv[t, k_len] = jnp.zeros((tile_len, tile_len), BF16)

    load_c.start()
    for c in range(2):
        for o in range(link_len):
            arrived_back[c][o][most] = jnp.zeros((part_rows[c], tile_len), BF16)
        ext[c][tiles] = jnp.zeros((part_rows[c], tile_len), BF16)

    load_f.wait()
    load_i.wait()
    for t in range(tiles):
        block = fields[:, :, t * fine : (t + 1) * fine].reshape(rows, fine)
        coarse[t] = dot_t(block, interp[t])
        for l in range(level_len):
            levels[wide + l, t] = coarse[t, pl.ds(l, members, stride=level_len), :]
    for i in range(wide // 2):
        low = jnp.concatenate([levels[wide + 2 * i], levels[wide + 2 * i + 1]], axis=1)
        top = level_len + 2 * i
        high = jnp.concatenate([levels[top], levels[top + 1]], axis=1)
        halo_out[0, i] = low.astype(BF16)
        halo_out[1, i] = high.astype(BF16)

    down = pltpu.make_async_remote_copy(
        halo_out.at[0],
        halo_in.at[1],
        halo_sem.at[0],
        halo_sem.at[1],
        device_id={"lev": lax.rem(me_l + n_lev - 1, n_lev)},
        device_id_type=MESH,
    )
    up = pltpu.make_async_remote_copy(
        halo_out.at[1],
        halo_in.at[0],
        halo_sem.at[2],
        halo_sem.at[3],
        device_id={"lev": lax.rem(me_l + 1, n_lev)},
        device_id_type=MESH,
    )
    start = me_l * level_len

    def coefficient(level, column):
        return weight[column, jnp.clip(start + level, 0, total_levels - 1)]

    def adjoint_level(level):
        value = coefficient(level - half, wide) * levels[wide + level - half]
        for e in range(1 - half, half + 1):
            value = value + coefficient(level + e, half - e) * levels[wide + level + e]
        if level < 0:
            value = jnp.where(start + level >= 0, value, 0.0)
        if level >= level_len:
            value = jnp.where(start + level < total_levels, value, 0.0)
        middle[half + level] = value

    def forward_pair(level):
        both = []
        for l in (level, level + 1):
            value = coefficient(l, 0) * middle[l]
            for j in range(1, wide + 1):
                value = value + coefficient(l, j) * middle[l + j]
            both.append(value)
        pair = jnp.concatenate(both, axis=1).astype(BF16)
        if wide <= level < level_len - wide:
            smooth[0][:, pl.ds((level - wide) * members, 2 * members), :] = pair
        else:
            place = level if level < wide else level - level_len + 2 * wide
            smooth[1][:, pl.ds(place * members, 2 * members), :] = pair

    for level in range(half, level_len - half):
        adjoint_level(level)
    for level in range(wide, level_len - wide, 2):
        forward_pair(level)

    load_c.wait()

    def gathered(left, first):
        right = jnp.concatenate(
            [
                jnp.concatenate([conv[t, which[t, first + s]] for t in range(tiles)], axis=1)
                for s in range(most)
            ],
            axis=0,
        )
        return dot_t(left, right)

    def side_by_side(ref, count):
        return jnp.concatenate([ref[i] for i in range(count)], axis=1)

    def sum_back(c, o):
        sums = gathered(side_by_side(smooth[c], tiles), tiles + o * most).astype(BF16)
        for s in range(most):
            returning[c][o][s] = sums[:, s * tile_len : (s + 1) * tile_len]

    def send_back(c, o):
        copy = pltpu.make_async_remote_copy(
            returning[c][o],
            arrived_back[c][o].at[pl.ds(0, most)],
            back_sem.at[0, c, o],
            back_sem.at[1, c, o],
            device_id={"patch": source[o]},
            device_id_type=MESH,
        )
        copy.start()
        return copy

    def sum_own(c):
        low = 0 if c == 0 else part_rows[0]
        left = side_by_side(smooth[c], tiles)
        for first in range(0, tiles, most):
            sums = gathered(left, first)
            for s in range(most):
                own[first + s, pl.ds(low, part_rows[c])] = sums[
                    :, s * tile_len : (s + 1) * tile_len
                ]

    def send_forth(c):
        low = 0 if c == 0 else part_rows[0]
        for t in range(tiles):
            value = own[t, low : low + part_rows[c]]
            for o in range(link_len):
                value = value + arrived_back[c][o][slot_of[t, o]].astype(F32)
            ext[c][t] = value.astype(BF16)
        copies = {}
        for o in order:
            for s in range(most):
                sending[c][o][s] = ext[c][send[0, s, o]]
            copies[o] = pltpu.make_async_remote_copy(
                sending[c][o],
                arrived[c][o],
                forth_sem.at[0, c, o],
                forth_sem.at[1, c, o],
                device_id={"patch": partner[o]},
                device_id_type=MESH,
            )
            copies[o].start()
        return copies

    def spread(left, first, count, t):
        right = jnp.concatenate(
            [
                jnp.concatenate([conv[u, which[u, first + e]] for e in range(count)], axis=0)
                for u in (t, t + 1)
            ],
            axis=1,
        )
        return jnp.dot(left, right, preferred_element_type=F32)

    def places(c):
        if c == 0:
            return [(0, part_rows[0], edge)]
        return [(0, edge, 0), (edge, edge, rows - edge)]

    def put(c, t, sums, fresh):
        for begin, count, place in places(c):
            for i in range(2):
                value = sums[begin : begin + count, i * tile_len : (i + 1) * tile_len]
                if not fresh:
                    value = value + mixed[t + i, pl.ds(place, count)]
                mixed[t + i, pl.ds(place, count)] = value

    def mix_own(c):
        left = side_by_side(ext[c], tiles)
        for t in range(0, tiles, 2):
            put(c, t, spread(left, 0, tiles, t), True)

    def mix_link(c, o):
        left = side_by_side(arrived[c][o], most)
        for t in range(0, tiles, 2):
            put(c, t, spread(left, tiles + o * most, most, t), False)

    for o in order:
        sum_back(0, o)
    beside = jnp.where(me_l > 0, 1, 0) + jnp.where(me_l < n_lev - 1, 1, 0)
    pl.semaphore_wait(barrier, link_len + beside)

    @pl.when(me_l > 0)
    def _():
        down.start()

    @pl.when(me_l < n_lev - 1)
    def _():
        up.start()

    back = [{o: send_back(0, o) for o in order}, {}]
    sum_own(0)

    def unpack(side, base):
        for i in range(wide // 2):
            pair = halo_in[side, i].astype(F32)
            levels[base + 2 * i] = pair[:, :members]
            levels[base + 2 * i + 1] = pair[:, members:]

    def clear(base):
        for i in range(wide):
            levels[base + i] = jnp.zeros(levels.shape[1:], F32)

    @pl.when(me_l > 0)
    def _():
        up.wait_recv()
        unpack(0, 0)

    @pl.when(me_l == 0)
    def _():
        clear(0)

    @pl.when(me_l < n_lev - 1)
    def _():
        down.wait_recv()
        unpack(1, wide + level_len)

    @pl.when(me_l == n_lev - 1)
    def _():
        clear(wide + level_len)

    for level in list(range(-half, half)) + list(range(level_len - half, level_len + half)):
        adjoint_level(level)
    for level in list(range(0, wide, 2)) + list(range(level_len - wide, level_len, 2)):
        forward_pair(level)

    for o in order:
        sum_back(1, o)
        back[1][o] = send_back(1, o)
    sum_own(1)
    forth = []
    for c in range(2):
        for o in order:
            back[c][o].wait_recv()
        forth.append(send_forth(c))
        mix_own(c)
    for c in range(2):
        for o in order[::-1]:
            forth[c][o].wait_recv()
            mix_link(c, o)
    for t in range(tiles):
        part = jnp.concatenate(
            [mixed[t, pl.ds(m, level_len, stride=members), :] for m in range(members)], axis=0
        ).astype(BF16)
        result = jnp.dot(part, interp[t], preferred_element_type=F32)
        out[:, :, t * fine : (t + 1) * fine] = result.reshape(members, level_len, fine)
    for copies in back + forth:
        for o in order:
            copies[o].wait_send()

    @pl.when(me_l > 0)
    def _():
        down.wait_send()

    @pl.when(me_l < n_lev - 1)
    def _():
        up.wait_send()


def solution(mesh):
    n_patch, n_lev = mesh.shape["patch"], mesh.shape["lev"]

    def shards(fields, interp, conv_weight, vert_weight, send_tiles, tile_pattern):
        members, level_len, column_len = fields.shape
        tiles, tile_len, fine = interp.shape
        k_len = conv_weight.shape[1]
        link_len, most = send_tiles.shape[1:]
        wide = vert_weight.shape[1] - 1
        rows = members * level_len
        any_spec = pl.BlockSpec(memory_space=pl.ANY)
        smem_spec = pl.BlockSpec(memory_space=pltpu.SMEM)

        edge = 2 * wide * members

        def per_part(count, copies):
            return [
                pltpu.VMEM((count, part_rows, tile_len), BF16)
                for part_rows in (rows - edge, edge)
                for _ in range(copies)
            ]

        return pl.pallas_call(
            functools.partial(kernel, n_patch, n_lev),
            name="localize",
            out_shape=pltpu.VMEM(fields.shape, F32),
            in_specs=[any_spec] * 3 + [smem_spec] * 3,
            out_specs=pl.BlockSpec(memory_space=pltpu.VMEM),
            scratch_shapes=[
                pltpu.VMEM(fields.shape, BF16),
                pltpu.VMEM(interp.shape, BF16),
                pltpu.VMEM((tiles, k_len + 1, tile_len, tile_len), BF16),
                pltpu.VMEM((tiles, rows, tile_len), F32),
                pltpu.VMEM((level_len + 2 * wide, tiles, members, tile_len), F32),
                pltpu.VMEM((level_len + wide, tiles, members, tile_len), F32),
                pltpu.VMEM((2, wide // 2, tiles, 2 * members, tile_len), BF16),
                pltpu.VMEM((2, wide // 2, tiles, 2 * members, tile_len), BF16),
                pltpu.VMEM((tiles, rows, tile_len), F32),
                pltpu.VMEM((tiles, rows, tile_len), F32),
                pltpu.SMEM((tiles, tiles + link_len * most), jnp.int32),
                pltpu.SMEM((tiles, link_len), jnp.int32),
                pltpu.SemaphoreType.DMA((3,)),
                pltpu.SemaphoreType.DMA((4,)),
                pltpu.SemaphoreType.DMA((2, 2, link_len)),
                pltpu.SemaphoreType.DMA((2, 2, link_len)),
            ]
            + per_part(tiles, 1)
            + per_part(tiles + 1, 1)
            + per_part(most, link_len)
            + per_part(most + 1, link_len)
            + per_part(most, link_len)
            + per_part(most, link_len),
            compiler_params=pltpu.CompilerParams(collective_id=0, has_side_effects=True),
        )(fields, interp, conv_weight, vert_weight.T, send_tiles.transpose(0, 2, 1), tile_pattern)

    in_specs = (
        P(None, "lev", "patch"),
        P("patch", None, None),
        P("patch", None, None, None),
        P(),
        P("patch", None, None),
        P("patch", None),
    )
    out_specs = P(None, "lev", "patch")
    return jax.shard_map(shards, mesh=mesh, in_specs=in_specs, out_specs=out_specs, check_vma=False)
```
